32 devices in a mesh: expert: 16 (over z, x, core), tensor: 2 (over y).
Axes of the slice: x: 2, y: 2, z: 4, core: 2. Of those that a mesh axis runs over, the one named last changes fastest.
Arguments:
- tokens: bfloat16 [1024, 2048], P('expert'), may hold values from -6 to 6
- expert_ids: int32 [1024, 6], replicated, may hold values from 0 to 31, all different within a row; in each aligned block of 1024 rows (0 to 1023, 1024 to 2047, ...) at most 256 rows name the same one
- gate_probs: float32 [1024, 6], replicated, may hold values from 0.02 to 0.6
- w_gate: bfloat16 [32, 2048, 1408], P('expert', None, 'tensor'), may hold values from -0.125 to 0.125
- w_up: bfloat16 [32, 2048, 1408], P('expert', None, 'tensor'), may hold values from -0.125 to 0.125
- w_down: bfloat16 [32, 1408, 2048], P('expert', 'tensor'), may hold values from -0.15625 to 0.15625
- shared_gate: bfloat16 [2048, 2816], P(None, 'tensor'), may hold values from -0.125 to 0.125
- shared_up: bfloat16 [2048, 2816], P(None, 'tensor'), may hold values from -0.125 to 0.125
- shared_down: bfloat16 [2816, 2048], P('tensor'), may hold values from -0.109375 to 0.109375
Outputs:
- layer_out: bfloat16 [1024, 2048], P('expert')
The draws below stay inside these ranges and needn't reach their ends.
Inputs may be any that keep to these rules, and one draw needn't show every extreme that they name: `expert_ids`: each row names 6 different experts. Over all 1024 tokens no expert is named more than 256 times, a bound that some block reaches.
All inputs are finite; a program needn't handle non-finite values.
Results may differ from the reference program's by a relative error of at most 0.011.
Values may be sent and summed in bfloat16 or wider, within the bound.
A program may use at most 64 MiB of HBM per device.

```python
import math
import jax
import jax.numpy as jnp
import numpy as np
from jax import lax

D = 2048
RF = 1408
SF = 2816
TOPK = 6
EXPERTS = 32
TOKENS = 1024
CAP = 256


def levels(rng, extent, cuts, least, top_value):
    def one(axis_at, shards_of):
        steps = jax.random.uniform(jax.random.fold_in(jax.random.fold_in(rng, 6), axis_at), (shards_of,), jnp.float32, least / len(cuts), top_value / len(cuts))
        return jnp.repeat(jnp.exp(steps), extent[axis_at] // shards_of).reshape((-1,) + (1,) * (len(extent) - axis_at - 1))

    loudness = one(*cuts[0])
    for cut in cuts[1:]:
        loudness = loudness * one(*cut)
    return loudness


def assign_block(rng, own, number, rows, amount, top, bound, slope):
    ranking = jax.random.permutation(rng, amount)
    packed, common = shares(amount, rows * top, bound, slope, True), shares(amount, rows * top, bound, slope, False)
    places = jnp.arange(amount)

    def named(lengths, rotation):
        used = int((lengths > 0).sum())
        fixed = max(1, used // 4)
        shifted = fixed + (places - fixed + rotation * (used - fixed)) % max(1, amount - fixed)
        return jnp.zeros((amount,), jnp.int32).at[ranking[jnp.where(places < fixed, places, shifted)]].set(jnp.asarray(lengths, jnp.int32))

    lengths = jnp.where(number % 4 == 0, named(packed, number // 4), named(common, number - number // 4 - 1))
    mixed = jax.random.permutation(jax.random.fold_in(own, 3), amount)
    source_of, taker = mixed[0:amount // 2 * 2:2], mixed[1:amount // 2 * 2:2]
    margin = jnp.minimum(lengths[source_of] - 1, bound - lengths[taker]) // 2
    margin = jnp.where((source_of == ranking[0]) | (taker == ranking[0]) | (lengths[taker] == 0), 0, jnp.maximum(margin, 0))
    shifted = jax.random.randint(jax.random.fold_in(own, 4), (amount // 2,), 0, 1 << 20) % (margin + 1)
    lengths = lengths.at[source_of].add(-shifted).at[taker].add(shifted)
    labels = jnp.searchsorted(jnp.cumsum(lengths), jnp.arange(rows * top), side="right").astype(jnp.int32)
    grid = labels.reshape(top, rows).T
    grid = grid[jax.random.permutation(jax.random.fold_in(own, 1), rows)]
    rotation = jax.random.randint(jax.random.fold_in(own, 2), (rows, 1), 0, top)
    return jnp.take_along_axis(grid, (jnp.arange(top)[None, :] + rotation) % top, axis=1)


def shares(number_of, total, most, skew, full):
    weights = [(1 << 20) // math.isqrt(grade ** skew) + 1 for grade in range(1, number_of + 1)]
    largest = most if full else min(most, max(-(-total // number_of), total * weights[0] // sum(weights)))
    least = 1 if total - largest >= number_of - 1 else 0
    holding, rest = [largest] + [least] * (number_of - 1), total - largest - least * (number_of - 1)
    while rest > 0:
        free = [i for i in range(1, number_of) if holding[i] < largest] or [i for i in range(1, number_of) if holding[i] < most]
        mass, budget = sum([weights[i] for i in free]), rest
        for i in free:
            addition = min(most - holding[i], max(1, budget * weights[i] // mass), rest)
            holding[i] = holding[i] + addition
            rest = rest - addition
    return np.array(holding)


def bell_draw(own_key, shape, scale, bound, split=(), kind=jnp.bfloat16):
    entries = scale * jax.random.normal(own_key, shape, jnp.float32)
    if split:
        entries = entries * levels(own_key, shape, split, -0.22, 0.18)
    return jnp.clip(entries, -bound, bound).astype(kind)


def setup_inputs(seed: int = 0) -> dict:
    arg_keys = jax.random.split(jax.random.key(seed), 10)
    tokens = bell_draw(arg_keys[0], (TOKENS, D), 1.0, 6.0, ((0, 16),))
    expert_ids_keys = jax.random.split(jax.random.fold_in(arg_keys[1], 1), TOKENS // TOKENS)
    expert_ids_turns = jax.random.permutation(jax.random.fold_in(arg_keys[1], 3), TOKENS // TOKENS)
    expert_ids = jax.vmap(lambda own, number: assign_block(jax.random.fold_in(arg_keys[1], 2), own, number, TOKENS, EXPERTS, TOPK, CAP, 2))(expert_ids_keys, expert_ids_turns).reshape((TOKENS, TOPK))
    gate_probs = jnp.clip(jnp.exp(jax.random.uniform(arg_keys[2], (TOKENS, TOPK), jnp.float32, math.log(0.02), math.log(0.6))), 0.02, 0.6)
    w_gate = bell_draw(arg_keys[3], (EXPERTS, D, RF), D ** -0.5, 0.125, ((0, 16), (2, 2)))
    w_up = bell_draw(arg_keys[4], (EXPERTS, D, RF), D ** -0.5, 0.125, ((0, 16), (2, 2)))
    w_down = bell_draw(arg_keys[5], (EXPERTS, RF, D), RF ** -0.5, 0.15625, ((0, 16), (1, 2)))
    shared_gate = bell_draw(arg_keys[6], (D, SF), D ** -0.5, 0.125, ((1, 2),))
    shared_up = bell_draw(arg_keys[7], (D, SF), D ** -0.5, 0.125, ((1, 2),))
    shared_down = bell_draw(arg_keys[8], (SF, D), SF ** -0.5, 0.109375, ((0, 2),))
    return {"tokens": tokens, "expert_ids": expert_ids, "gate_probs": gate_probs, "w_gate": w_gate, "w_up": w_up, "w_down": w_down, "shared_gate": shared_gate, "shared_up": shared_up, "shared_down": shared_down}


def reference(tokens, expert_ids, gate_probs, w_gate, w_up, w_down, shared_gate, shared_up, shared_down):
    flat_ids = expert_ids.reshape(-1)
    onehot = (flat_ids[:, None] == jnp.arange(EXPERTS, dtype=jnp.int32)[None, :]).astype(jnp.int32)
    before = jnp.cumsum(onehot, axis=0) - onehot
    slot = jnp.sum(before * onehot, axis=1).reshape(expert_ids.shape).astype(jnp.int32)
    positions = jnp.arange(CAP, dtype=jnp.int32)

    def one_expert(total, inputs):
        gate_w, up_w, down_w, expert = inputs
        hits = expert_ids == expert
        target = jnp.sum(jnp.where(hits, slot + 1, 0), axis=1) - 1
        weight = jnp.sum(jnp.where(hits, gate_probs, 0.0), axis=1)
        picker = (positions[:, None] == target[None, :]).astype(jnp.bfloat16)
        dispatched = jnp.dot(picker, tokens, preferred_element_type=jnp.float32).astype(jnp.bfloat16)
        gate = jnp.dot(dispatched, gate_w, preferred_element_type=jnp.float32)
        upper = jnp.dot(dispatched, up_w, preferred_element_type=jnp.float32)
        hidden = (jax.nn.silu(gate) * upper).astype(jnp.bfloat16)
        slot_out = jnp.dot(hidden, down_w, preferred_element_type=jnp.float32)
        back = jnp.dot(picker.astype(jnp.float32).T, slot_out, precision=lax.Precision.HIGHEST)
        return total + weight[:, None] * back, None

    start = jnp.zeros(tokens.shape, jnp.float32)
    routed, _ = lax.scan(one_expert, start, (w_gate, w_up, w_down, jnp.arange(EXPERTS, dtype=jnp.int32)))
    sgate = jnp.dot(tokens, shared_gate, preferred_element_type=jnp.float32)
    supper = jnp.dot(tokens, shared_up, preferred_element_type=jnp.float32)
    shared_hidden = (jax.nn.silu(sgate) * supper).astype(jnp.bfloat16)
    shared = jnp.dot(shared_hidden, shared_down, preferred_element_type=jnp.float32)
    return (shared + routed).astype(jnp.bfloat16)
```

```python
import functools
import math

import jax
import jax.numpy as jnp
from jax import lax
from jax.experimental import pallas as pl
from jax.experimental.pallas import tpu as pltpu
from jax.sharding import PartitionSpec as P

MESH = pl.DeviceIdType.MESH


def here(width):
    e = lax.axis_index("expert")
    return lax.div(e, 4), lax.rem(lax.div(e, 2), 2), lax.rem(e, 2), lax.axis_index("tensor")


def expert_at(line, side, core):
    return (line * 2 + side) * 2 + core


def peers_of(t, width):
    return [lax.rem(t + j, width) for j in range(1, width)]


def barrier(z, x, c, t, lines, width):
    sem = pltpu.get_barrier_semaphore()

    def greet(**where):
        pl.semaphore_signal(sem, inc=1, device_id=where, device_id_type=MESH)

    @pl.when(z > 0)
    def _():
        greet(expert=expert_at(z - 1, x, c))

    @pl.when(z < lines - 1)
    def _():
        greet(expert=expert_at(z + 1, x, c))

    greet(expert=expert_at(z, 1 - x, c))
    greet(expert=expert_at(z, x, 1 - c))
    for p in peers_of(t, width):
        greet(tensor=p)

    pl.semaphore_wait(sem, 1 + width + lax.min(z, 1) + lax.min(lines - 1 - z, 1))


def remote(src, dst, send, recv, **where):
    return pltpu.make_async_remote_copy(
        src_ref=src, dst_ref=dst, send_sem=send, recv_sem=recv, device_id=where, device_id_type=MESH
    )


def ring_of(z, k, lines):
    if k == 0:
        return [(z, None)]
    return [(z - k, z - k >= 0), (z + k, z + k < lines)]


def guarded(cond, fn):
    if cond is None:
        fn()
    else:
        pl.when(cond)(fn)


def gather_kernel(lines, width, x_ref, out, own_sem, z_send, z_recv, x_send, x_recv, y_send, y_recv, c_send, c_recv):
    z, x, c, t = here(width)
    barrier(z, x, c, t, lines, width)
    me = expert_at(z, x, c)

    def own(line):
        return out.at[expert_at(line, x, c)]

    def line_copy(src, line, up):
        to = z + 1 if up else z - 1
        d = 1 if up else 0
        return remote(src, own(line), z_send.at[d, line], z_recv.at[d, line], expert=expert_at(to, x, c))

    def side_copy(src, line, side):
        return remote(
            src, out.at[expert_at(line, side, c), t], x_send.at[line], x_recv.at[line],
            expert=expert_at(z, 1 - x, c),
        )

    def wide_copy(line, part, j, slot):
        ref = out.at[expert_at(line, 1 - x, c), part]
        return remote(ref, ref, y_send.at[line, j], y_recv.at[line, slot], tensor=lax.rem(t + j + 1, width))

    def core_copy(src, line, side, core):
        return remote(
            src, out.at[expert_at(line, side, core)], c_send.at[line, side], c_recv.at[line, side],
            expert=expert_at(z, x, 1 - c),
        )

    keep = pltpu.make_async_copy(x_ref, out.at[me], own_sem)
    keep.start()

    def first(line, k):
        def go():
            src = x_ref if k == 0 else own(line)

            def send_up():
                line_copy(src, line, True).start()

            def send_down():
                line_copy(src, line, False).start()

            if k == 0:
                pl.when(z < lines - 1)(send_up)
                pl.when(z > 0)(send_down)
            side_copy(src.at[t], line, x).start()
            core_copy(src, line, x, c).start()

        return go

    def arrive(line, k, from_below):
        def go():
            line_copy(own(line), line, from_below).wait_recv()
            if from_below:
                pl.when(z < lines - 1)(lambda: line_copy(own(line), line, True).start())
            else:
                pl.when(z > 0)(lambda: line_copy(own(line), line, False).start())
            side_copy(own(line).at[t], line, x).start()
            core_copy(own(line), line, x, c).start()

        return go

    for k in range(lines + 2):
        if k < lines:
            for i, (line, ok) in enumerate(ring_of(z, k, lines)):
                guarded(ok, first(line, 0) if k == 0 else arrive(line, k, i == 0))
        if 1 <= k <= lines:
            for line, ok in ring_of(z, k - 1, lines):

                def pass_on(line=line):
                    side_copy(out.at[expert_at(line, 1 - x, c), t], line, 1 - x).wait_recv()
                    for j in range(width - 1):
                        wide_copy(line, t, j, j).start()

                guarded(ok, pass_on)
        if k >= 2:
            for line, ok in ring_of(z, k - 2, lines):

                def to_core(line=line):
                    for j in range(width - 1):
                        part = lax.rem(t + 2 * width - j - 1, width)
                        wide_copy(line, part, j, j).wait_recv()
                    core_copy(out.at[expert_at(line, 1 - x, c)], line, 1 - x, c).start()

                guarded(ok, to_core)

    keep.wait()
    for line in range(lines):
        for side in range(2):
            core_copy(out.at[expert_at(line, side, 1 - c)], line, side, 1 - c).wait()
        side_copy(out.at[expert_at(line, x, c), t], line, x).wait_send()
        for j in range(width - 1):
            wide_copy(line, t, j, j).wait_send()
        pl.when((z < lines - 1) & (line <= z))(lambda line=line: line_copy(own(line), line, True).wait_send())
        pl.when((z > 0) & (line >= z))(lambda line=line: line_copy(own(line), line, False).wait_send())


def gather(tokens, experts, width):
    rows, depth = tokens.shape
    lines = experts // 4
    part = rows // width
    dma = pltpu.SemaphoreType.DMA
    out = pl.pallas_call(
        functools.partial(gather_kernel, lines, width),
        out_shape=jax.ShapeDtypeStruct((experts, width, part, depth), tokens.dtype),
        in_specs=[pl.BlockSpec(memory_space=pltpu.VMEM)],
        out_specs=pl.BlockSpec(memory_space=pltpu.VMEM),
        scratch_shapes=[
            dma,
            dma((2, lines)),
            dma((2, lines)),
            dma((lines,)),
            dma((lines,)),
            dma((lines, max(1, width - 1))),
            dma((lines, max(1, width - 1))),
            dma((lines, 2)),
            dma((lines, 2)),
        ],
        compiler_params=pltpu.CompilerParams(collective_id=0, has_side_effects=True),
    )(tokens.reshape(width, part, depth))
    return out.reshape(experts * rows, depth)


def combine_kernel(
    lines, width, p_ref, s_ref, o_ref, cin, aout, yin, xout, xin, zout, zin, fin,
    c_send, c_recv, y_send, y_recv, x_send, x_recv, z_send, z_recv, f_send, f_recv,
):
    z, x, c, t = here(width)
    f32, half = jnp.float32, jnp.bfloat16
    barrier(z, x, c, t, lines, width)

    def core_copy(line, side):
        return remote(
            p_ref.at[expert_at(line, side, 1 - c)], cin.at[line, side], c_send.at[line, side], c_recv.at[line, side],
            expert=expert_at(z, x, 1 - c),
        )

    def wide_copy(line, j):
        to = lax.rem(t + j + 1, width)
        return remote(aout.at[line, to], yin.at[line, j], y_send.at[line, j], y_recv.at[line, j], tensor=to)

    def side_copy(line):
        return remote(xout.at[line], xin.at[line], x_send.at[line], x_recv.at[line], expert=expert_at(z, 1 - x, c))

    def line_copy(line, up):
        d = 1 if up else 0
        to = z + 1 if up else z - 1
        return remote(zout.at[line], zin.at[d, line], z_send.at[line], z_recv.at[d, line], expert=expert_at(to, x, c))

    def last_copy(j):
        to = lax.rem(t + j + 1, width)
        return remote(fin.at[t], fin.at[t], f_send.at[j], f_recv.at[j], tensor=to)

    order = [ring_of(z, k, lines) for k in range(lines - 1, -1, -1)]
    for level in order:
        for side in (1 - x, x):
            for line, ok in level:
                guarded(ok, lambda line=line, side=side: core_copy(line, side).start())

    def other_side(line):
        core_copy(line, 1 - x).wait_recv()
        aout[line] = (p_ref[expert_at(line, 1 - x, c)].astype(f32) + cin[line, 1 - x].astype(f32)).astype(half)
        for j in range(width - 1):
            wide_copy(line, j).start()

    def cross(line):
        acc = aout[line, t].astype(f32)
        for j in range(width - 1):
            wide_copy(line, j).wait_recv()
            acc = acc + yin[line, j].astype(f32)
        xout[line] = acc.astype(half)
        side_copy(line).start()

    def near(line, dst):
        core_copy(line, x).wait_recv()
        dst[line] = (p_ref[expert_at(line, x, c)].astype(f32) + cin[line, x].astype(f32)).astype(half)
        side_copy(line).wait_recv()
        dst[line, t] = (
            p_ref[expert_at(line, x, c), t].astype(f32) + cin[line, x, t].astype(f32) + xin[line].astype(f32)
        ).astype(half)

    def onward(line, up):
        near(line, zout)

        def add():
            line_copy(line, up).wait_recv()
            zout[line] = (zout[line].astype(f32) + zin[1 if up else 0, line].astype(f32)).astype(half)

        pl.when(z > 0 if up else z < lines - 1)(add)
        line_copy(line, up).start()

    def finish():
        near(z, zout)
        fin[t] = (zout[z].astype(f32) + s_ref[...]).astype(half)
        for up in (False, True):

            def add(up=up):
                line_copy(z, up).wait_recv()
                fin[t] = (fin[t].astype(f32) + zin[1 if up else 0, z].astype(f32)).astype(half)

            pl.when(z > 0 if up else z < lines - 1)(add)
        for j in range(width - 1):
            last_copy(j).start()

    for k in range(lines + 2):
        if k < lines:
            for line, ok in order[k]:
                guarded(ok, functools.partial(other_side, line))
        if 1 <= k <= lines:
            for line, ok in order[k - 1]:
                guarded(ok, functools.partial(cross, line))
        if k >= 2:
            level = order[k - 2]
            if len(level) == 1:
                finish()
            else:
                for i, (line, ok) in enumerate(level):
                    guarded(ok, functools.partial(onward, line, i == 1))

    for j in range(width - 1):
        part = lax.rem(t + 2 * width - j - 1, width)
        remote(fin.at[part], fin.at[part], f_send.at[j], f_recv.at[j], tensor=part).wait_recv()
    acc = fin[0].astype(f32)
    for j in range(1, width):
        acc = acc + fin[j].astype(f32)
    o_ref[...] = acc.astype(half)

    for j in range(width - 1):
        last_copy(j).wait_send()
    for line in range(lines):
        for side in range(2):
            core_copy(line, side).wait_send()
        for j in range(width - 1):
            wide_copy(line, j).wait_send()
        side_copy(line).wait_send()
        pl.when(line != z)(lambda line=line: line_copy(line, True).wait_send())


def combine(partial, shared, experts, width):
    total, depth = partial.shape
    rows = total // experts
    part = rows // width
    lines = experts // 4
    peers = max(1, width - 1)
    dma = pltpu.SemaphoreType.DMA
    half = jnp.bfloat16
    block = (width, part, depth)
    vmem = pl.BlockSpec(memory_space=pltpu.VMEM)
    out = pl.pallas_call(
        functools.partial(combine_kernel, lines, width),
        out_shape=jax.ShapeDtypeStruct(block, half),
        in_specs=[vmem, vmem],
        out_specs=vmem,
        scratch_shapes=[
            pltpu.VMEM((lines, 2) + block, half),
            pltpu.VMEM((lines,) + block, half),
            pltpu.VMEM((lines, peers, part, depth), half),
            pltpu.VMEM((lines, part, depth), half),
            pltpu.VMEM((lines, part, depth), half),
            pltpu.VMEM((lines,) + block, half),
            pltpu.VMEM((2, lines) + block, half),
            pltpu.VMEM((width,) + block, half),
            dma((lines, 2)),
            dma((lines, 2)),
            dma((lines, peers)),
            dma((lines, peers)),
            dma((lines,)),
            dma((lines,)),
            dma((lines,)),
            dma((2, lines)),
            dma((peers,)),
            dma((peers,)),
        ],
        compiler_params=pltpu.CompilerParams(collective_id=1, has_side_effects=True),
    )(partial.reshape((experts,) + block), shared.reshape(block))
    return out.reshape(rows, depth)


def place_rows(expert_ids, gate_probs, expert):
    hits = expert_ids == expert
    row_hit = jnp.sum(hits.astype(jnp.float32), axis=1)
    total_rows = row_hit.shape[0]
    block = math.gcd(total_rows, 128)
    blocks = row_hit.reshape(total_rows // block, block)
    lower = jnp.arange(block, dtype=jnp.int32)
    strict = (lower[:, None] < lower[None, :]).astype(jnp.float32)
    inside = jnp.dot(blocks, strict, precision=lax.Precision.HIGHEST)
    sums = jnp.sum(blocks, axis=1)
    offsets = jnp.cumsum(sums) - sums
    before = (inside + offsets[:, None]).reshape(total_rows)
    target = jnp.where(row_hit > 0.5, before, -1.0).astype(jnp.int32)
    weight = jnp.sum(jnp.where(hits, gate_probs, 0.0), axis=1)
    return (target, weight)


def body(experts, width, tokens, expert_ids, gate_probs, w_gate, w_up, w_down, shared_gate, shared_up, shared_down):
    f32, half = jnp.float32, jnp.bfloat16
    local_count = w_gate.shape[0]
    capacity = 4 * tokens.shape[0]
    first_expert = lax.axis_index("expert") * local_count
    local_experts = first_expert + jnp.arange(local_count, dtype=jnp.int32)
    everyone = gather(tokens, experts, width)
    targets, weights = jax.vmap(lambda expert: place_rows(expert_ids, gate_probs, expert))(local_experts)
    positions = jnp.arange(capacity, dtype=jnp.int32)
    hit = positions[None, :, None] == targets[:, None, :]
    slot_weight = jnp.sum(jnp.where(hit, weights[:, None, :], 0.0), axis=2)
    picker = hit.astype(half)
    dispatched = jnp.einsum("lcr,rd->lcd", picker, everyone, preferred_element_type=f32).astype(half)
    gate = jnp.einsum("lcd,ldf->lcf", dispatched, w_gate, preferred_element_type=f32)
    upper = jnp.einsum("lcd,ldf->lcf", dispatched, w_up, preferred_element_type=f32)
    hidden = (jax.nn.silu(gate) * upper * slot_weight[:, :, None]).astype(half)
    slot_out = jnp.einsum("lcf,lfd->lcd", hidden, w_down, preferred_element_type=f32).astype(half)
    partial = jnp.einsum("lcr,lcd->rd", picker, slot_out, preferred_element_type=f32).astype(half)
    sgate = jnp.dot(tokens, shared_gate, preferred_element_type=f32)
    supper = jnp.dot(tokens, shared_up, preferred_element_type=f32)
    shared_hidden = (jax.nn.silu(sgate) * supper).astype(half)
    shared = jnp.dot(shared_hidden, shared_down, preferred_element_type=f32)
    return combine(partial, shared, experts, width)


def solution(mesh):
    placed = (
        P("expert", None),
        P(),
        P(),
        P("expert", None, "tensor"),
        P("expert", None, "tensor"),
        P("expert", "tensor", None),
        P(None, "tensor"),
        P(None, "tensor"),
        P("tensor", None),
    )
    experts, width = mesh.shape["expert"], mesh.shape["tensor"]
    return jax.shard_map(
        functools.partial(body, experts, width),
        mesh=mesh, in_specs=placed, out_specs=P("expert", None), check_vma=False,
    )
```

```python
import functools
import math

import jax
import jax.numpy as jnp
from jax import lax
from jax.experimental import pallas as pl
from jax.experimental.pallas import tpu as pltpu
from jax.sharding import PartitionSpec as P

MESH = pl.DeviceIdType.MESH


def here(width):
    e = lax.axis_index("expert")
    return lax.div(e, 4), lax.rem(lax.div(e, 2), 2), lax.rem(e, 2), lax.axis_index("tensor")


def expert_at(line, side, core):
    return (line * 2 + side) * 2 + core


def peers_of(t, width):
    return [lax.rem(t + j, width) for j in range(1, width)]


def barrier(z, x, c, t, lines, width):
    sem = pltpu.get_barrier_semaphore()

    def greet(**where):
        pl.semaphore_signal(sem, inc=1, device_id=where, device_id_type=MESH)

    @pl.when(z > 0)
    def _():
        greet(expert=expert_at(z - 1, x, c))

    @pl.when(z < lines - 1)
    def _():
        greet(expert=expert_at(z + 1, x, c))

    greet(expert=expert_at(z, 1 - x, c))
    greet(expert=expert_at(z, x, 1 - c))
    for p in peers_of(t, width):
        greet(tensor=p)

    pl.semaphore_wait(sem, 1 + width + lax.min(z, 1) + lax.min(lines - 1 - z, 1))


def remote(src, dst, send, recv, **where):
    return pltpu.make_async_remote_copy(
        src_ref=src, dst_ref=dst, send_sem=send, recv_sem=recv, device_id=where, device_id_type=MESH
    )


def ring_of(z, k, lines):
    if k == 0:
        return [(z, None)]
    return [(z - k, z - k >= 0), (z + k, z + k < lines)]


def guarded(cond, fn):
    if cond is None:
        fn()
    else:
        pl.when(cond)(fn)


def gather_kernel(lines, width, x_ref, flat_ref, sg_hbm, su_hbm, sd_hbm, out, s_ref, sg, su, sd, w_sem, own_sem, z_send, z_recv, x_send, x_recv, y_send, y_recv, c_send, c_recv):
    z, x, c, t = here(width)
    loads = [
        pltpu.make_async_copy(src, dst, w_sem.at[i])
        for i, (src, dst) in enumerate(((sg_hbm, sg), (su_hbm, su), (sd_hbm, sd)))
    ]
    for load in loads:
        load.start()
    barrier(z, x, c, t, lines, width)
    me = expert_at(z, x, c)
    hidden = sg.shape[1]
    cuts = [(i, min(256, hidden - i)) for i in range(0, hidden, 256)]

    def shared_piece(i):
        at, size = cuts[i]
        f32 = jnp.float32
        g = jnp.dot(flat_ref[...], sg[:, at : at + size], preferred_element_type=f32)
        u = jnp.dot(flat_ref[...], su[:, at : at + size], preferred_element_type=f32)
        h = (g / (1.0 + jnp.exp(-g)) * u).astype(jnp.bfloat16)
        depth = s_ref.shape[1]
        step = math.gcd(depth, 512)
        for n in range(0, depth, step):
            piece = jnp.dot(h, sd[at : at + size, n : n + step], preferred_element_type=f32)
            s_ref[:, n : n + step] = piece if i == 0 else s_ref[:, n : n + step] + piece

    def own(line):
        return out.at[expert_at(line, x, c)]

    def line_copy(src, line, up):
        to = z + 1 if up else z - 1
        d = 1 if up else 0
        return remote(src, own(line), z_send.at[d, line], z_recv.at[d, line], expert=expert_at(to, x, c))

    def side_copy(src, line, side):
        return remote(
            src, out.at[expert_at(line, side, c), t], x_send.at[line], x_recv.at[line],
            expert=expert_at(z, 1 - x, c),
        )

    def wide_copy(line, part, j, slot):
        ref = out.at[expert_at(line, 1 - x, c), part]
        return remote(ref, ref, y_send.at[line, j], y_recv.at[line, slot], tensor=lax.rem(t + j + 1, width))

    def core_copy(src, line, side, core):
        return remote(
            src, out.at[expert_at(line, side, core)], c_send.at[line, side], c_recv.at[line, side],
            expert=expert_at(z, x, 1 - c),
        )

    keep = pltpu.make_async_copy(x_ref, out.at[me], own_sem)
    keep.start()

    def first(line, k):
        def go():
            src = x_ref if k == 0 else own(line)

            def send_up():
                line_copy(src, line, True).start()

            def send_down():
                line_copy(src, line, False).start()

            if k == 0:
                pl.when(z < lines - 1)(send_up)
                pl.when(z > 0)(send_down)
            side_copy(src.at[t], line, x).start()
            core_copy(src, line, x, c).start()

        return go

    def arrive(line, k, from_below):
        def go():
            line_copy(own(line), line, from_below).wait_recv()
            if from_below:
                pl.when(z < lines - 1)(lambda: line_copy(own(line), line, True).start())
            else:
                pl.when(z > 0)(lambda: line_copy(own(line), line, False).start())
            side_copy(own(line).at[t], line, x).start()
            core_copy(own(line), line, x, c).start()

        return go

    for k in range(lines + 2):
        if k < lines:
            for i, (line, ok) in enumerate(ring_of(z, k, lines)):
                guarded(ok, first(line, 0) if k == 0 else arrive(line, k, i == 0))
        if 1 <= k <= lines:
            for line, ok in ring_of(z, k - 1, lines):

                def pass_on(line=line):
                    side_copy(out.at[expert_at(line, 1 - x, c), t], line, 1 - x).wait_recv()
                    for j in range(width - 1):
                        wide_copy(line, t, j, j).start()

                guarded(ok, pass_on)
        if k >= 2:
            for line, ok in ring_of(z, k - 2, lines):

                def to_core(line=line):
                    for j in range(width - 1):
                        part = lax.rem(t + 2 * width - j - 1, width)
                        wide_copy(line, part, j, j).wait_recv()
                    core_copy(out.at[expert_at(line, 1 - x, c)], line, 1 - x, c).start()

                guarded(ok, to_core)
        if k == 1:
            for load in loads:
                load.wait()
        for i in range(len(cuts)):
            if k == 1 + i * max(1, lines - 1) // len(cuts):
                shared_piece(i)

    keep.wait()
    for line in range(lines):
        for side in range(2):
            core_copy(out.at[expert_at(line, side, 1 - c)], line, side, 1 - c).wait()
        side_copy(out.at[expert_at(line, x, c), t], line, x).wait_send()
        for j in range(width - 1):
            wide_copy(line, t, j, j).wait_send()
        pl.when((z < lines - 1) & (line <= z))(lambda line=line: line_copy(own(line), line, True).wait_send())
        pl.when((z > 0) & (line >= z))(lambda line=line: line_copy(own(line), line, False).wait_send())


def gather(tokens, shared_gate, shared_up, shared_down, experts, width):
    rows, depth = tokens.shape
    lines = experts // 4
    part = rows // width
    dma = pltpu.SemaphoreType.DMA
    vmem, hbm = pl.BlockSpec(memory_space=pltpu.VMEM), pl.BlockSpec(memory_space=pltpu.HBM)
    out, shared = pl.pallas_call(
        functools.partial(gather_kernel, lines, width),
        out_shape=(
            jax.ShapeDtypeStruct((experts, width, part, depth), tokens.dtype),
            jax.ShapeDtypeStruct((rows, depth), jnp.float32),
        ),
        in_specs=[vmem, vmem, hbm, hbm, hbm],
        out_specs=(vmem, vmem),
        scratch_shapes=[
            pltpu.VMEM(shared_gate.shape, shared_gate.dtype),
            pltpu.VMEM(shared_up.shape, shared_up.dtype),
            pltpu.VMEM(shared_down.shape, shared_down.dtype),
            dma((3,)),
            dma,
            dma((2, lines)),
            dma((2, lines)),
            dma((lines,)),
            dma((lines,)),
            dma((lines, max(1, width - 1))),
            dma((lines, max(1, width - 1))),
            dma((lines, 2)),
            dma((lines, 2)),
        ],
        compiler_params=pltpu.CompilerParams(collective_id=0, has_side_effects=True),
    )(tokens.reshape(width, part, depth), tokens, shared_gate, shared_up, shared_down)
    return out.reshape(experts * rows, depth), shared


def combine_kernel(
    lines, width, sel_ref, slot_ref, s_ref, o_ref, p_ref, cin, aout, yin, xout, xin, zout, zin, fin,
    c_send, c_recv, y_send, y_recv, x_send, x_recv, z_send, z_recv, f_send, f_recv,
):
    z, x, c, t = here(width)
    f32, half = jnp.float32, jnp.bfloat16
    barrier(z, x, c, t, lines, width)

    def core_copy(line, side):
        return remote(
            p_ref.at[expert_at(line, side, 1 - c)], cin.at[line, side], c_send.at[line, side], c_recv.at[line, side],
            expert=expert_at(z, x, 1 - c),
        )

    def wide_copy(line, j):
        to = lax.rem(t + j + 1, width)
        return remote(aout.at[line, to], yin.at[line, j], y_send.at[line, j], y_recv.at[line, j], tensor=to)

    def side_copy(line):
        return remote(xout.at[line], xin.at[line], x_send.at[line], x_recv.at[line], expert=expert_at(z, 1 - x, c))

    def line_copy(line, up):
        d = 1 if up else 0
        to = z + 1 if up else z - 1
        return remote(zout.at[line], zin.at[d, line], z_send.at[line], z_recv.at[d, line], expert=expert_at(to, x, c))

    def last_copy(j):
        to = lax.rem(t + j + 1, width)
        return remote(fin.at[t], fin.at[t], f_send.at[j], f_recv.at[j], tensor=to)

    order = [ring_of(z, k, lines) for k in range(lines - 1, -1, -1)]

    def produce(line, side):
        row = line * 2 + side
        depth = slot_ref.shape[1]
        step = math.gcd(depth, 512)
        block = p_ref.shape[1:3]
        for n in range(0, depth, step):
            piece = jnp.dot(sel_ref[row], slot_ref[:, n : n + step], preferred_element_type=f32)
            piece = piece.reshape((2,) + block + (step,)).astype(half)
            p_ref[pl.ds(row * 2, 2), :, :, n : n + step] = piece
        core_copy(line, side).start()

    def other_side(line):
        core_copy(line, 1 - x).wait_recv()
        aout[line] = (p_ref[expert_at(line, 1 - x, c)].astype(f32) + cin[line, 1 - x].astype(f32)).astype(half)
        for j in range(width - 1):
            wide_copy(line, j).start()

    def cross(line):
        acc = aout[line, t].astype(f32)
        for j in range(width - 1):
            wide_copy(line, j).wait_recv()
            acc = acc + yin[line, j].astype(f32)
        xout[line] = acc.astype(half)
        side_copy(line).start()

    def near(line, dst):
        core_copy(line, x).wait_recv()
        dst[line] = (p_ref[expert_at(line, x, c)].astype(f32) + cin[line, x].astype(f32)).astype(half)
        side_copy(line).wait_recv()
        dst[line, t] = (
            p_ref[expert_at(line, x, c), t].astype(f32) + cin[line, x, t].astype(f32) + xin[line].astype(f32)
        ).astype(half)

    def onward(line, up):
        near(line, zout)

        def add():
            line_copy(line, up).wait_recv()
            zout[line] = (zout[line].astype(f32) + zin[1 if up else 0, line].astype(f32)).astype(half)

        pl.when(z > 0 if up else z < lines - 1)(add)
        line_copy(line, up).start()

    def finish():
        near(z, zout)
        fin[t] = (zout[z].astype(f32) + s_ref[...]).astype(half)
        for up in (False, True):

            def add(up=up):
                line_copy(z, up).wait_recv()
                fin[t] = (fin[t].astype(f32) + zin[1 if up else 0, z].astype(f32)).astype(half)

            pl.when(z > 0 if up else z < lines - 1)(add)
        for j in range(width - 1):
            last_copy(j).start()

    for k in range(lines + 3):
        if k < lines:
            for side in (1 - x, x):
                for line, ok in order[k]:
                    guarded(ok, functools.partial(produce, line, side))
        if 1 <= k <= lines:
            for line, ok in order[k - 1]:
                guarded(ok, functools.partial(other_side, line))
        if 2 <= k <= lines + 1:
            for line, ok in order[k - 2]:
                guarded(ok, functools.partial(cross, line))
        if k >= 3:
            level = order[k - 3]
            if len(level) == 1:
                finish()
            else:
                for i, (line, ok) in enumerate(level):
                    guarded(ok, functools.partial(onward, line, i == 1))

    for j in range(width - 1):
        part = lax.rem(t + 2 * width - j - 1, width)
        remote(fin.at[part], fin.at[part], f_send.at[j], f_recv.at[j], tensor=part).wait_recv()
    acc = fin[0].astype(f32)
    for j in range(1, width):
        acc = acc + fin[j].astype(f32)
    o_ref[...] = acc.astype(half)

    for j in range(width - 1):
        last_copy(j).wait_send()
    for line in range(lines):
        for side in range(2):
            core_copy(line, side).wait_send()
        for j in range(width - 1):
            wide_copy(line, j).wait_send()
        side_copy(line).wait_send()
        pl.when(line != z)(lambda line=line: line_copy(line, True).wait_send())


def combine(chosen, slot_out, shared, experts, width):
    total, depth = chosen.shape[0], slot_out.shape[1]
    rows = total // experts
    part = rows // width
    lines = experts // 4
    peers = max(1, width - 1)
    dma = pltpu.SemaphoreType.DMA
    half = jnp.bfloat16
    block = (width, part, depth)
    vmem = pl.BlockSpec(memory_space=pltpu.VMEM)
    out = pl.pallas_call(
        functools.partial(combine_kernel, lines, width),
        out_shape=jax.ShapeDtypeStruct(block, half),
        in_specs=[vmem, vmem, vmem],
        out_specs=vmem,
        scratch_shapes=[
            pltpu.VMEM((experts,) + block, half),
            pltpu.VMEM((lines, 2) + block, half),
            pltpu.VMEM((lines,) + block, half),
            pltpu.VMEM((lines, peers, part, depth), half),
            pltpu.VMEM((lines, part, depth), half),
            pltpu.VMEM((lines, part, depth), half),
            pltpu.VMEM((lines,) + block, half),
            pltpu.VMEM((2, lines) + block, half),
            pltpu.VMEM((width,) + block, half),
            dma((lines, 2)),
            dma((lines, 2)),
            dma((lines, peers)),
            dma((lines, peers)),
            dma((lines,)),
            dma((lines,)),
            dma((lines,)),
            dma((2, lines)),
            dma((peers,)),
            dma((peers,)),
        ],
        compiler_params=pltpu.CompilerParams(collective_id=1, has_side_effects=True),
    )(chosen.reshape(experts // 2, 2 * rows, -1), slot_out, shared.reshape(block))
    return out.reshape(rows, depth)


def place_rows(expert_ids, gate_probs, expert):
    hits = expert_ids == expert
    row_hit = jnp.sum(hits.astype(jnp.float32), axis=1)
    total_rows = row_hit.shape[0]
    block = math.gcd(total_rows, 128)
    blocks = row_hit.reshape(total_rows // block, block)
    lower = jnp.arange(block, dtype=jnp.int32)
    strict = (lower[:, None] < lower[None, :]).astype(jnp.float32)
    inside = jnp.dot(blocks, strict, precision=lax.Precision.HIGHEST)
    sums = jnp.sum(blocks, axis=1)
    offsets = jnp.cumsum(sums) - sums
    before = (inside + offsets[:, None]).reshape(total_rows)
    target = jnp.where(row_hit > 0.5, before, -1.0).astype(jnp.int32)
    weight = jnp.sum(jnp.where(hits, gate_probs, 0.0), axis=1)
    return (target, weight)


def body(experts, width, tokens, expert_ids, gate_probs, w_gate, w_up, w_down, shared_gate, shared_up, shared_down):
    f32, half = jnp.float32, jnp.bfloat16
    local_count = w_gate.shape[0]
    capacity = 4 * tokens.shape[0]
    first_expert = lax.axis_index("expert") * local_count
    local_experts = first_expert + jnp.arange(local_count, dtype=jnp.int32)
    everyone, shared = gather(tokens, shared_gate, shared_up, shared_down, experts, width)
    targets, weights = jax.vmap(lambda expert: place_rows(expert_ids, gate_probs, expert))(local_experts)
    positions = jnp.arange(capacity, dtype=jnp.int32)
    hit = positions[None, :, None] == targets[:, None, :]
    slot_weight = jnp.sum(jnp.where(hit, weights[:, None, :], 0.0), axis=2)
    picker = hit.astype(half)
    dispatched = jnp.einsum("lcr,rd->lcd", picker, everyone, preferred_element_type=f32).astype(half)
    gate = jnp.einsum("lcd,ldf->lcf", dispatched, w_gate, preferred_element_type=f32)
    upper = jnp.einsum("lcd,ldf->lcf", dispatched, w_up, preferred_element_type=f32)
    hidden = (jax.nn.silu(gate) * upper * slot_weight[:, :, None]).astype(half)
    slot_out = jnp.einsum("lcf,lfd->lcd", hidden, w_down, preferred_element_type=f32).astype(half)
    columns = jnp.arange(local_count * capacity, dtype=jnp.int32)
    chosen = False
    for i in range(local_count):
        place = jnp.where(targets[i] >= 0, targets[i] + i * capacity, -1)
        chosen = chosen | (place[:, None] == columns[None, :])
    chosen = chosen.astype(half)
    return combine(chosen, slot_out.reshape(local_count * capacity, -1), shared, experts, width)


def solution(mesh):
    placed = (
        P("expert", None),
        P(),
        P(),
        P("expert", None, "tensor"),
        P("expert", None, "tensor"),
        P("expert", "tensor", None),
        P(None, "tensor"),
        P(None, "tensor"),
        P("tensor", None),
    )
    experts, width = mesh.shape["expert"], mesh.shape["tensor"]
    return jax.shard_map(
        functools.partial(body, experts, width),
        mesh=mesh, in_specs=placed, out_specs=P("expert", None), check_vma=False,
    )
```
